256 devices in a mesh: ep: 8 (over y_lo, x), fsdp: 32 (over z, y_hi, core).
Axes of the slice: x: 4, y: 4 (y_hi: 2, y_lo: 2; y = y_hi * 2 + y_lo), z: 8, core: 2. Of those that a mesh axis runs over, the one named last changes fastest.
Arguments:
- train_gate: float32 [64, 2048, 1408], P('ep', 'fsdp'), may hold values from -0.25 to 0.25
- train_up: float32 [64, 2048, 1408], P('ep', 'fsdp'), may hold values from -0.25 to 0.25
- train_down: float32 [64, 1408, 2048], P('ep', None, 'fsdp'), may hold values from -0.3125 to 0.3125
- router_weight: float32 [2048, 64], P('fsdp', 'ep'), may hold values from -0.125 to 0.125
- router_gain: float32 [2048], P('fsdp'), may hold values from 0.25 to 1.75
Outputs:
- ready_gate: bfloat16 [64, 2048, 1408], P('ep', None, 'fsdp')
- ready_up: bfloat16 [64, 2048, 1408], P('ep', None, 'fsdp')
- ready_down: bfloat16 [64, 1408, 2048], P('ep', 'fsdp')
- scale_gate: float32 [64, 1408], P('ep', 'fsdp')
- scale_up: float32 [64, 1408], P('ep', 'fsdp')
- scale_down: float32 [64, 1408], P('ep', 'fsdp')
- serve_router: bfloat16 [2048, 64], replicated
The draws below stay inside these ranges and needn't reach their ends.
All inputs are finite; a program needn't handle non-finite values. Where the reference program divides by a largest or mean magnitude, that divisor is 1e-20 or more.
Results may differ from the reference program's by a relative error of at most 0.001.
Values may be sent and summed in bfloat16 or wider, within the bound.
A program may use at most 128 MiB of HBM per device.

```python
import jax
import jax.numpy as jnp

EXPERTS = 64
D_MODEL = 2048
D_EXPERT = 1408


def with_spikes(result, rng, source, target, shards_of, factor):
    def block_of(dim):
        return (jnp.arange(result.shape[dim]) // (result.shape[dim] // shards_of)).reshape((-1,) + (1,) * (result.ndim - 1 - dim))

    near = jax.random.permutation(rng, shards_of)[block_of(target)]
    other_side = (block_of(target) + shards_of // 2) % shards_of
    return jnp.where((block_of(source) == near) | (block_of(source) == other_side), factor * result, result)


def shard_levels(key, dims, pieces, low, largest):
    level, own = 1.0, jax.random.fold_in(key, 6)
    for position, shards_of in pieces:
        steps = jnp.exp(jax.random.uniform(jax.random.fold_in(own, position), (shards_of,), jnp.float32, low / len(pieces), largest / len(pieces)))
        level = level * jnp.repeat(steps, dims[position] // shards_of).reshape([-1 if axis == position else 1 for axis in range(len(dims))])
    return level


def centred(rng, shape, deviation, most, shards=(), kind=jnp.bfloat16):
    result = deviation * jax.random.normal(rng, shape, jnp.float32)
    if shards:
        result = result * shard_levels(rng, shape, shards, -0.22, 0.18)
    return jnp.clip(result, -most, most).astype(kind)


def bell_draw_with(own_key, shape, width, reach, shards, heavy, held_as=jnp.bfloat16):
    drawn = width * jax.random.normal(own_key, shape, jnp.float32)
    if shards:
        drawn = drawn * shard_levels(own_key, shape, shards, -0.22, 0.18)
    return jnp.clip(with_spikes(drawn, jax.random.fold_in(own_key, 3), *heavy), -reach, reach).astype(held_as)


def setup_inputs(seed: int = 0) -> dict:
    keys = jax.random.split(jax.random.key(seed), 6)
    train_gate = bell_draw_with(keys[0], (EXPERTS, D_MODEL, D_EXPERT), D_MODEL ** -0.5, 0.25, ((0, 8), (1, 32)), (1, 2, 32, 2.75), jnp.float32)
    train_up = bell_draw_with(keys[1], (EXPERTS, D_MODEL, D_EXPERT), D_MODEL ** -0.5, 0.25, ((0, 8), (1, 32)), (1, 2, 32, 2.75), jnp.float32)
    train_down = bell_draw_with(keys[2], (EXPERTS, D_EXPERT, D_MODEL), D_EXPERT ** -0.5, 0.3125, ((0, 8), (2, 32)), (2, 1, 32, 2.75), jnp.float32)
    router_weight = centred(keys[3], (D_MODEL, EXPERTS), D_MODEL ** -0.5, 0.125, ((0, 32), (1, 8)), jnp.float32)
    router_gain = jnp.clip(1.0 + 0.15 * jax.random.normal(keys[4], (D_MODEL,), jnp.float32), 0.25, 1.75)
    return {"train_gate": train_gate, "train_up": train_up, "train_down": train_down, "router_weight": router_weight, "router_gain": router_gain}


def reference(train_gate, train_up, train_down, router_weight, router_gain):
    scale_gate = jnp.max(jnp.abs(train_gate), axis=1)
    ready_gate = (train_gate / jnp.expand_dims(scale_gate, 1)).astype(jnp.bfloat16)
    scale_up = jnp.max(jnp.abs(train_up), axis=1)
    ready_up = (train_up / jnp.expand_dims(scale_up, 1)).astype(jnp.bfloat16)
    scale_down = jnp.max(jnp.abs(train_down), axis=2)
    ready_down = (train_down / jnp.expand_dims(scale_down, 2)).astype(jnp.bfloat16)
    serve_router = (router_weight * router_gain[:, None]).astype(jnp.bfloat16)
    return ready_gate, ready_up, ready_down, scale_gate, scale_up, scale_down, serve_router
```

```python
import jax
import jax.numpy as jnp
from jax import lax
from jax.experimental import pallas as pl
from jax.experimental.pallas import tpu as pltpu
from jax.sharding import PartitionSpec as P

MESH = pl.DeviceIdType.MESH
N = 32
EP = 8
E, D, J = 8, 64, 1408
JT = J // 128
JD = J // N
ROWS = JD * E // 2
GROUPS = 4
PIECE = 384


def exchange(
    gate, up, down, rw, rg, land, scales, router,
    x, stage, sent, own_max, got_max, own_scale, all_scale, recip, rhalf, rtile,
    load_sem, rsend, rrecv, asend, arecv, dsend, drecv, dself,
    csend, crecv, zsend, zrecv, ysend, yrecv, esend, erecv, eself, out_sem,
):
    me = lax.axis_index("fsdp")
    ep = lax.axis_index("ep")
    z, yh, core = me // 4, lax.rem(me // 2, 2), lax.rem(me, 2)

    loads = []
    for m, ref in enumerate((gate, up, down)):
        loads.append(pltpu.make_async_copy(ref, x.at[m], load_sem.at[m]))
        loads[m].start()

    barrier = pltpu.get_barrier_semaphore()

    def greet(d, _):
        pl.semaphore_signal(barrier, inc=1, device_id={"fsdp": lax.rem(me + d, N)}, device_id_type=MESH)
        return 0

    def greet_ep(d, _):
        pl.semaphore_signal(barrier, inc=1, device_id={"ep": lax.rem(ep + d, EP)}, device_id_type=MESH)
        return 0

    lax.fori_loop(1, N, greet, 0)
    lax.fori_loop(1, EP, greet_ep, 0)

    part = rw[...] * rg[...]
    rhalf[0] = jnp.concatenate([part, part], axis=1)

    def maxima(m):
        def one(e, _):
            top = jnp.max(jnp.abs(x[m, e]), axis=0, keepdims=True)
            for g in range(GROUPS):
                w = min(PIECE, J - g * PIECE)
                own_max[m, e * GROUPS + g, :, :w] = top[:, g * PIECE : g * PIECE + w]
            return 0

        lax.fori_loop(0, E, one, 0)

    def send_maxima(m):
        def one(d, _):
            to = lax.rem(me + d, N)
            pltpu.make_async_remote_copy(
                own_max.at[m, to], got_max.at[m, me], rsend.at[m], rrecv.at[m], device_id={"fsdp": to}, device_id_type=MESH
            ).start()
            return 0

        lax.fori_loop(1, N, one, 0)

    def wait_bytes(ref, sem):
        pltpu.make_async_copy(ref, ref, sem).wait()

    def send_scales(m):
        got_max[m, me] = own_max[m, me]
        wait_bytes(got_max.at[m, pl.ds(0, N - 1)], rrecv.at[m])
        own_scale[m] = jnp.max(got_max[m], axis=0)
        all_scale[m, me] = own_scale[m]

        def one(d, _):
            to = lax.rem(me + d, N)
            pltpu.make_async_remote_copy(
                own_scale.at[m], all_scale.at[m, me], asend.at[m], arecv.at[m], device_id={"fsdp": to}, device_id_type=MESH
            ).start()
            return 0

        lax.fori_loop(1, N, one, 0)

    def send_matrix(m):
        wait_bytes(all_scale.at[m, pl.ds(0, N - 1)], arecv.at[m])
        for e in range(E):
            for g in range(GROUPS):
                recip[e : e + 1, g * PIECE : (g + 1) * PIECE] = 1.0 / all_scale[m, e * GROUPS + g]

        def tile(q, _):
            at = pl.multiple_of(q * 128, 128)
            for r in range(E // 2):
                v = x[m, 2 * r : 2 * r + 2, :, pl.ds(at, 128)] * recip[2 * r : 2 * r + 2, pl.ds(at, 128)][:, None, :]
                stage[pl.ds(r, 128, stride=E // 2), :] = v.reshape(128, 128).T
            sent[m, pl.ds(pl.multiple_of(q * 512, 512), 512), :] = stage[...].astype(jnp.bfloat16)
            return 0

        lax.fori_loop(0, JT, tile, 0)

        def rows_of(to):
            return sent.at[m, pl.ds(pl.multiple_of(to * ROWS, ROWS), ROWS)]

        def one(d, _):
            to = lax.rem(me + d, N)
            pltpu.make_async_remote_copy(
                rows_of(to), land.at[m, me], dsend.at[m], drecv.at[m], device_id={"fsdp": to}, device_id_type=MESH
            ).start()
            return 0

        lax.fori_loop(1, N, one, 0)
        pltpu.make_async_copy(rows_of(me), land.at[m, me], dself.at[m]).start()

    loads[0].wait()
    maxima(0)
    pl.semaphore_wait(barrier, N - 1 + EP - 1)
    send_maxima(0)
    router_core = pltpu.make_async_remote_copy(
        rhalf.at[0], rhalf.at[1], csend, crecv, device_id={"fsdp": me + 1 - 2 * core}, device_id_type=MESH
    )
    router_core.start()
    loads[1].wait()
    maxima(1)
    send_maxima(1)
    loads[2].wait()
    maxima(2)
    send_maxima(2)

    router_core.wait()
    lane = lax.broadcasted_iota(jnp.int32, (E, 128), 1)
    own_side = (lane // 64) == core
    rtile[yh, z] = jnp.where(own_side, rhalf[0], rhalf[1]).astype(jnp.bfloat16)

    def router_z(d, _):
        pltpu.make_async_remote_copy(
            rtile.at[yh, z], rtile.at[yh, z], zsend, zrecv,
            device_id={"fsdp": lax.rem(me + 4 * d, N)}, device_id_type=MESH,
        ).start()
        return 0

    lax.fori_loop(1, 8, router_z, 0)

    send_scales(0)
    send_scales(1)
    send_scales(2)
    send_matrix(0)

    wait_bytes(rtile.at[0, pl.ds(0, 7)], zrecv)
    router_y = pltpu.make_async_remote_copy(
        rtile.at[yh], rtile.at[yh], ysend, yrecv, device_id={"fsdp": me + 2 - 4 * yh}, device_id_type=MESH
    )
    router_y.start()
    send_matrix(1)
    router_y.wait_recv()

    def router_ep(d, _):
        for half in range(2):
            pltpu.make_async_remote_copy(
                rtile.at[half], router.at[ep, :, half], esend, erecv,
                device_id={"ep": lax.rem(ep + d, EP)}, device_id_type=MESH,
            ).start()
        return 0

    lax.fori_loop(1, EP, router_ep, 0)
    for half in range(2):
        pltpu.make_async_copy(rtile.at[half], router.at[ep, :, half], eself.at[half]).start()
    send_matrix(2)

    keep = pltpu.make_async_copy(all_scale, scales, out_sem)
    keep.start()
    wait_bytes(rtile.at[0, pl.ds(0, 7)], zsend)
    router_y.wait_send()
    wait_bytes(router.at[pl.ds(0, EP - 1)], esend)
    wait_bytes(router.at[pl.ds(0, EP - 1)], erecv)
    for half in range(2):
        pltpu.make_async_copy(rtile.at[half], router.at[ep, :, half], eself.at[half]).wait()
    for m in range(3):
        wait_bytes(own_max.at[m, pl.ds(0, N - 1)], rsend.at[m])
        wait_bytes(all_scale.at[m, pl.ds(0, N - 1)], asend.at[m])
    keep.wait()
    for m in range(3):
        pltpu.make_async_copy(sent.at[m, pl.ds(0, ROWS)], land.at[m, me], dself.at[m]).wait()
        wait_bytes(sent.at[m, pl.ds(0, (N - 1) * ROWS)], dsend.at[m])
        wait_bytes(land.at[m, pl.ds(0, N - 1)], drecv.at[m])


def merge(land, gate, up, down, rows):
    low = lax.broadcasted_iota(jnp.int32, (16, 128), 1) < 64
    for m, out in enumerate((gate, up, down)):
        for c in range(N // 2):
            a = land[m, 2 * c].astype(jnp.float32)
            b = land[m, 2 * c + 1].astype(jnp.float32)
            rows[m, c, pl.ds(0, 16, stride=2), :] = jnp.where(low, a, pltpu.roll(b, 64, 1))
            rows[m, c, pl.ds(1, 16, stride=2), :] = jnp.where(low, pltpu.roll(a, 64, 1), b)
        for c in range(N // 2):
            out[:, :, c * 128 : (c + 1) * 128] = rows[m, c].astype(jnp.bfloat16).reshape(4, E, 128)


def per_device(train_gate, train_up, train_down, router_weight, router_gain):
    f32, bf16 = jnp.float32, jnp.bfloat16
    anywhere = pl.BlockSpec(memory_space=pl.ANY)
    vmem = pl.BlockSpec(memory_space=pltpu.VMEM)
    dma = pltpu.SemaphoreType.DMA
    land, scales, router = pl.pallas_call(
        exchange,
        out_shape=(
            jax.ShapeDtypeStruct((3, N, ROWS, 128), bf16),
            jax.ShapeDtypeStruct((3, N, 1, PIECE), f32),
            jax.ShapeDtypeStruct((EP, 8, 2, E, 128), bf16),
        ),
        in_specs=[anywhere] * 3 + [vmem] * 2,
        out_specs=(anywhere,) * 3,
        scratch_shapes=[
            pltpu.VMEM((3, E, D, J), f32),
            pltpu.VMEM((512, 128), f32),
            pltpu.VMEM((3, N * ROWS, 128), bf16),
            pltpu.VMEM((3, N, 1, PIECE), f32),
            pltpu.VMEM((3, N, 1, PIECE), f32),
            pltpu.VMEM((3, 1, PIECE), f32),
            pltpu.VMEM((3, N, 1, PIECE), f32),
            pltpu.VMEM((E, GROUPS * PIECE), f32),
            pltpu.VMEM((2, E, 128), f32),
            pltpu.VMEM((2, 8, E, 128), bf16),
        ]
        + [dma((3,))] * 8
        + [dma] * 8
        + [dma((2,)), dma],
        compiler_params=pltpu.CompilerParams(collective_id=0, has_side_effects=True, vmem_limit_bytes=60 * 2**20),
        name="exchange",
    )(
        train_gate,
        train_up,
        jnp.transpose(train_down, (0, 2, 1)),
        jnp.transpose(router_weight),
        router_gain[None, :],
    )
    ready = jax.ShapeDtypeStruct((JD, E, D * N), bf16)
    block = pl.BlockSpec((4, E, D * N), lambda i: (i, 0, 0))
    gate, up, down = pl.pallas_call(
        merge,
        grid=(JD // 4,),
        out_shape=(ready,) * 3,
        in_specs=[pl.BlockSpec((3, N, 16, 128), lambda i: (0, 0, i, 0))],
        out_specs=(block,) * 3,
        scratch_shapes=[pltpu.VMEM((3, N // 2, 32, 128), f32)],
        compiler_params=pltpu.CompilerParams(dimension_semantics=("arbitrary",)),
        name="merge",
    )(land)
    at = lax.axis_index("fsdp") * JD
    mine = lax.dynamic_slice_in_dim(scales.reshape(3, E, GROUPS * PIECE), at, JD, 2)
    serve = jnp.transpose(router, (0, 3, 1, 2, 4)).reshape(EP * E, D * N)
    return (
        jnp.transpose(gate, (1, 2, 0)),
        jnp.transpose(up, (1, 2, 0)),
        jnp.transpose(down, (1, 0, 2)),
        mine[0],
        mine[1],
        mine[2],
        jnp.transpose(serve),
    )


def solution(mesh):
    placed = (
        P("ep", "fsdp", None),
        P("ep", "fsdp", None),
        P("ep", None, "fsdp"),
        P("fsdp", "ep"),
        P("fsdp"),
    )
    return jax.shard_map(
        per_device,
        mesh=mesh,
        in_specs=placed,
        out_specs=(
            P("ep", None, "fsdp"),
            P("ep", None, "fsdp"),
            P("ep", "fsdp", None),
            P("ep", "fsdp"),
            P("ep", "fsdp"),
            P("ep", "fsdp"),
            P(),
        ),
        check_vma=False,
    )
```

```python
import jax
import jax.numpy as jnp
from jax import lax
from jax.experimental import pallas as pl
from jax.experimental.pallas import tpu as pltpu
from jax.sharding import PartitionSpec as P

MESH = pl.DeviceIdType.MESH
N = 32
EP = 8
E, D, J = 8, 64, 1408
JT = J // 128
JD = J // N
ROWS = JD * E // 2
CJ = 128 // E
LINES = -(-JD // CJ)
WIDE = J + 128
FAR_FIRST = (4, 3, 5, 2, 6, 1, 7, 0)
ARRIVAL = (0, 4, 3, 5, 2, 6, 1, 7)
EARLY = 4

LEVELS, STEPS, LOWEST = 30720, 128, 120


def encode(x, per_unit):
    n = jnp.floor(jnp.abs(x) * per_unit + 0.5)
    high = jnp.floor(n * (1 / STEPS))
    v = jnp.exp2(high - LOWEST) * (1.0 + (n - STEPS * high) * (1 / STEPS))
    return jnp.where(x < 0, -v, v)


def decode(v):
    size = jnp.abs(v)
    high = jnp.floor(jnp.log2(size))
    n = (high + (LOWEST - 1.0)) * STEPS + size * jnp.exp2(-high) * STEPS
    return jnp.where(v < 0, -n, n)


def exchange(
    gate, up, down, rw, rg, gate_out, up_out, down_out, scales, router,
    x, stage, sent, land, rows, tops, spread, recip, lines, got_lines, inv, fac, rw_v, rg_v, rhalf, rtile,
    load_sem, rload, lsend, lrecv, dsend, drecv, dself,
    csend, crecv, zsend, zrecv, ysend, yrecv, esend, erecv, eself,
):
    me = lax.axis_index("fsdp")
    ep = lax.axis_index("ep")
    z, yh, core = me // 4, lax.rem(me // 2, 2), lax.rem(me, 2)
    first = (JT * me) // N
    lane = lax.broadcasted_iota(jnp.int32, (E, 128), 1)
    row = lax.broadcasted_iota(jnp.int32, (E, 128), 0)

    loads = []
    for m, ref in enumerate((gate, up, down)):
        loads.append(pltpu.make_async_copy(ref, x.at[m], load_sem.at[m]))
        loads[m].start()
    rloads = [pltpu.make_async_copy(a, b, rload.at[i]) for i, (a, b) in enumerate(((rw, rw_v), (rg, rg_v)))]
    for load in rloads:
        load.start()

    barrier = pltpu.get_barrier_semaphore()

    def greet(d, _):
        pl.semaphore_signal(barrier, inc=1, device_id={"fsdp": lax.rem(me + d, N)}, device_id_type=MESH)
        return 0

    def greet_ep(d, _):
        pl.semaphore_signal(barrier, inc=1, device_id={"ep": lax.rem(ep + d, EP)}, device_id_type=MESH)
        return 0

    lax.fori_loop(1, N, greet, 0)
    lax.fori_loop(1, EP, greet_ep, 0)

    def wait_bytes(ref, sem):
        pltpu.make_async_copy(ref, ref, sem).wait()

    def maxima(m):
        def one(e, _):
            tops[m, pl.ds(e, 1), :J] = jnp.max(jnp.abs(x[m, e]), axis=0, keepdims=True)
            return 0

        tops[m, :, J:] = jnp.zeros((E, WIDE - J), jnp.float32)
        lax.fori_loop(0, E, one, 0)

    def scaling(m):
        top = tops[m]
        recip[...] = jnp.where(top > 1e-30, LEVELS / jnp.maximum(top, 1e-30), 0.0)

    def listed(values, i):
        found = 0
        for at, value in enumerate(values):
            found = jnp.where(i == at, value, found)
        return found

    def lay_out(m, i):
        q = lax.rem(first + i, JT)
        at = pl.multiple_of(q * 128, 128)
        for r in range(E // 2):
            v = encode(x[m, 2 * r : 2 * r + 2, :, pl.ds(at, 128)], recip[2 * r : 2 * r + 2, pl.ds(at, 128)][:, None, :])
            stage[pl.ds(r, 128, stride=E // 2), :] = v.reshape(128, 128).T
        sent[m, pl.ds(pl.multiple_of(q * 512, 512), 512), :] = stage[...].astype(jnp.bfloat16)

    def rows_of(m, to):
        return sent.at[m, pl.ds(pl.multiple_of(to * ROWS, ROWS), ROWS)]

    def send_rows(m, to):
        @pl.when(to != me)
        def _():
            pltpu.make_async_remote_copy(
                rows_of(m, to), land.at[m, me], dsend.at[m], drecv.at[m, me], device_id={"fsdp": to}, device_id_type=MESH
            ).start()

        @pl.when(to == me)
        def _():
            pltpu.make_async_copy(rows_of(m, to), land.at[m, me], dself.at[m]).start()

    def send_tile(m, i):
        q = lax.rem(first + i, JT)
        to = (N * q) // JT

        @pl.when(jnp.logical_or(i > 0, (JT * to) // N >= q))
        def _():
            send_rows(m, to)

        for more in (1, 2):

            @pl.when(to + more < (N * (q + 1)) // JT)
            def _():
                send_rows(m, to + more)

    def tiles(m, start, stop, make=True, send=True):
        def one(i, _):
            if make:
                lay_out(m, i)
            if send:
                send_tile(m, i)
            return 0

        lax.fori_loop(start, stop, one, 0)

    def send_last(m):
        to = (N * first) // JT

        @pl.when((JT * to) // N < first)
        def _():
            send_rows(m, to)

    def send_far_first(m):
        lax.fori_loop(0, JT, lambda i, _: (lay_out(m, i), 0)[1], 0)

        def one(i, _):
            to = 4 * lax.rem(z + listed(FAR_FIRST, i // 4), 8) + lax.rem(me + i, 4)
            send_rows(m, to)
            return 0

        lax.fori_loop(0, N, one, 0)

    own_lanes = (lane // CJ) == row

    def draw_lines(m):
        for e in range(E):
            spread[e : e + 1, :] = pltpu.roll(tops[m, e : e + 1], CJ * e, 1)

        def one(to, _):
            for g in range(LINES):
                c0 = JD * to + CJ * g
                at = pl.multiple_of((c0 // 128) * 128, 128)
                near = pltpu.roll(spread[:, pl.ds(at, 256)], 256 - lax.rem(c0, 128), 1)[:, :128]
                g0 = (LINES * m + g) * 128
                lines[to, :, g0 : g0 + 128] = jnp.sum(jnp.where(own_lanes, near, 0.0), axis=0, keepdims=True)
            return 0

        lax.fori_loop(0, N, one, 0)

    loads[0].wait()
    maxima(0)
    scaling(0)
    tiles(0, 0, EARLY, send=False)
    pl.semaphore_wait(barrier, N - 1 + EP - 1)
    tiles(0, 0, EARLY, make=False)
    tiles(0, EARLY, JT)
    send_last(0)

    for load in rloads:
        load.wait()
    part = rw_v[...] * rg_v[...]
    rhalf[0] = jnp.concatenate([part, part], axis=1)
    router_core = pltpu.make_async_remote_copy(
        rhalf.at[0], rhalf.at[1], csend, crecv, device_id={"fsdp": me + 1 - 2 * core}, device_id_type=MESH
    )
    router_core.start()
    loads[1].wait()
    loads[2].wait()
    maxima(1)
    maxima(2)
    draw_lines(0)
    draw_lines(1)
    draw_lines(2)
    got_lines[me] = lines[me]

    def send_line(d, _):
        to = lax.rem(me + d, N)
        pltpu.make_async_remote_copy(
            lines.at[to], got_lines.at[me], lsend, lrecv, device_id={"fsdp": to}, device_id_type=MESH
        ).start()
        return 0

    lax.fori_loop(1, N, send_line, 0)

    router_core.wait()
    own_side = (lane // 64) == core
    rtile[yh, z] = jnp.where(own_side, rhalf[0], rhalf[1]).astype(jnp.bfloat16)

    def router_z(d, _):
        pltpu.make_async_remote_copy(
            rtile.at[yh, z], rtile.at[yh, z], zsend, zrecv,
            device_id={"fsdp": lax.rem(me + 4 * d, N)}, device_id_type=MESH,
        ).start()
        return 0

    lax.fori_loop(1, 8, router_z, 0)

    scaling(1)
    send_far_first(1)

    scaling(2)
    send_far_first(2)
    wait_bytes(rtile.at[0, pl.ds(0, 7)], zrecv)
    router_y = pltpu.make_async_remote_copy(
        rtile.at[yh], rtile.at[yh], ysend, yrecv, device_id={"fsdp": me + 2 - 4 * yh}, device_id_type=MESH
    )
    router_y.start()
    wait_bytes(got_lines.at[pl.ds(0, N - 1)], lrecv)
    router_y.wait_recv()

    def router_ep(d, _):
        for half in range(2):
            pltpu.make_async_remote_copy(
                rtile.at[half], router.at[ep, :, half], esend, erecv,
                device_id={"ep": lax.rem(ep + d, EP)}, device_id_type=MESH,
            ).start()
        return 0

    lax.fori_loop(1, EP, router_ep, 0)
    for half in range(2):
        pltpu.make_async_copy(rtile.at[half], router.at[ep, :, half], eself.at[half]).start()

    def side_by_side(a, b):
        low = lax.broadcasted_iota(jnp.int32, (ROWS, 128), 1) < 64
        rows[pl.ds(0, ROWS, stride=2), :] = jnp.where(low, a, pltpu.roll(b, 64, 1))
        rows[pl.ds(1, ROWS, stride=2), :] = jnp.where(low, pltpu.roll(a, 64, 1), b)
        return rows[...]

    def by_expert(line):
        line = jnp.broadcast_to(line, (E, 128))
        for_each = line
        for e in range(1, E):
            for_each = jnp.where(row == e, pltpu.roll(line, 128 - CJ * e, 1), for_each)
        return for_each

    def line_at(m, g):
        return pl.ds((LINES * m + g) * 128, 128)

    def merge(m, out):
        scale = jnp.zeros((E, 128), jnp.float32)
        for g in range(LINES):
            part = by_expert(jnp.max(got_lines[:, :, line_at(m, g)], axis=0))
            inv[g] = (1 / LEVELS) / jnp.where(part > 0, part, 1.0)
            scale = jnp.where(lane // CJ == g, pltpu.roll(part, CJ * g, 1), scale)
        scales[m] = scale
        pltpu.make_async_copy(rows_of(m, me), land.at[m, me], dself.at[m]).wait()
        low = lane < 64

        def chip(i, _):
            c = 2 * lax.rem(z + listed(ARRIVAL, i // 2), 8) + lax.rem(yh + i, 2)
            for g in range(LINES):
                per = [
                    by_expert(got_lines[2 * c + side, :, line_at(m, g)]) * inv[g] for side in range(2)
                ]
                for j in range(min(CJ, JD - CJ * g)):
                    a, b = (jnp.broadcast_to(p[:, j : j + 1], (E, 128)) for p in per)
                    fac[(CJ * g + j) * E : (CJ * g + j + 1) * E, :] = jnp.where(low, a, b)
            for side in range(2):

                @pl.when(2 * c + side != me)
                def _():
                    wait_bytes(land.at[m, 2 * c + side], drecv.at[m, 2 * c + side])

            a, b = (decode(land[m, 2 * c + side].astype(jnp.float32)) for side in range(2))
            v = (side_by_side(a, b) * fac[...]).astype(jnp.bfloat16)
            out[:, :, pl.ds(pl.multiple_of(c * 128, 128), 128)] = v.reshape(JD, E, 128)
            return 0

        lax.fori_loop(0, N // 2, chip, 0)

    merge(0, gate_out)
    wait_bytes(rtile.at[0, pl.ds(0, 7)], zsend)
    router_y.wait_send()
    wait_bytes(router.at[pl.ds(0, EP - 1)], esend)
    wait_bytes(router.at[pl.ds(0, EP - 1)], erecv)
    for half in range(2):
        pltpu.make_async_copy(rtile.at[half], router.at[ep, :, half], eself.at[half]).wait()
    merge(1, up_out)
    merge(2, down_out)
    wait_bytes(lines.at[pl.ds(0, N - 1)], lsend)
    for m in range(3):
        wait_bytes(sent.at[m, pl.ds(0, (N - 1) * ROWS)], dsend.at[m])


def finish(gate, up, down, scales, router, gate_out, up_out, down_out, sg, su, sd, router_out, cut, sem):
    copies = [
        pltpu.make_async_copy(a, b, sem.at[i])
        for i, (a, b) in enumerate(((gate, gate_out), (up, up_out), (down, down_out), (router, router_out)))
    ]
    for copy in copies:
        copy.start()
    cut[...] = scales[:, :, :JD]
    small = [pltpu.make_async_copy(cut.at[m], out, sem.at[4 + m]) for m, out in enumerate((sg, su, sd))]
    for copy in small:
        copy.start()
    for copy in copies + small:
        copy.wait()


def per_device(train_gate, train_up, train_down, router_weight, router_gain):
    f32, bf16 = jnp.float32, jnp.bfloat16
    hbm = pl.BlockSpec(memory_space=pltpu.HBM)
    vmem = pl.BlockSpec(memory_space=pltpu.VMEM)
    dma = pltpu.SemaphoreType.DMA

    def stay(a):
        return pltpu.with_memory_space_constraint(a, pltpu.HBM)

    ready = jax.ShapeDtypeStruct((JD, E, D * N), bf16)
    gate, up, down, scales, router = pl.pallas_call(
        exchange,
        out_shape=(
            *(ready,) * 3,
            jax.ShapeDtypeStruct((3, E, 128), f32),
            jax.ShapeDtypeStruct((EP, 8, 2, E, 128), bf16),
        ),
        in_specs=[hbm] * 5,
        out_specs=(vmem,) * 5,
        scratch_shapes=[
            pltpu.VMEM((3, E, D, J), f32),
            pltpu.VMEM((512, 128), f32),
            pltpu.VMEM((3, N * ROWS, 128), bf16),
            pltpu.VMEM((3, N, ROWS, 128), bf16),
            pltpu.VMEM((JD * E, 128), f32),
            pltpu.VMEM((3, E, WIDE), f32),
            pltpu.VMEM((E, WIDE), f32),
            pltpu.VMEM((E, WIDE), f32),
            pltpu.VMEM((N, 1, 3 * LINES * 128), f32),
            pltpu.VMEM((N, 1, 3 * LINES * 128), f32),
            pltpu.VMEM((LINES, E, 128), f32),
            pltpu.VMEM((JD * E, 128), f32),
            pltpu.VMEM((E, D), f32),
            pltpu.VMEM((1, D), f32),
            pltpu.VMEM((2, E, 128), f32),
            pltpu.VMEM((2, 8, E, 128), bf16),
        ]
        + [dma((3,)), dma((2,))]
        + [dma] * 2
        + [dma((3,)), dma((3, N)), dma((3,))]
        + [dma] * 8
        + [dma((2,))],
        compiler_params=pltpu.CompilerParams(collective_id=0, has_side_effects=True, vmem_limit_bytes=40 * 2**20),
        name="exchange",
    )(
        stay(train_gate),
        stay(train_up),
        stay(jnp.transpose(train_down, (0, 2, 1))),
        stay(jnp.transpose(router_weight)),
        stay(router_gain[None, :]),
    )
    scale = jax.ShapeDtypeStruct((E, JD), f32)
    gate, up, down, scale_gate, scale_up, scale_down, router = pl.pallas_call(
        finish,
        out_shape=(*(ready,) * 3, *(scale,) * 3, jax.ShapeDtypeStruct((EP, 8, 2, E, 128), bf16)),
        in_specs=[vmem] * 5,
        out_specs=(hbm,) * 7,
        scratch_shapes=[pltpu.VMEM((3, E, JD), f32), dma((7,))],
        compiler_params=pltpu.CompilerParams(vmem_limit_bytes=16 * 2**20),
        name="finish",
    )(gate, up, down, scales, router)
    serve = jnp.transpose(router, (0, 3, 1, 2, 4)).reshape(EP * E, D * N)
    return (
        jnp.transpose(gate, (1, 2, 0)),
        jnp.transpose(up, (1, 2, 0)),
        jnp.transpose(down, (1, 0, 2)),
        scale_gate,
        scale_up,
        scale_down,
        jnp.transpose(serve),
    )


def solution(mesh):
    placed = (
        P("ep", "fsdp", None),
        P("ep", "fsdp", None),
        P("ep", None, "fsdp"),
        P("fsdp", "ep"),
        P("fsdp"),
    )
    return jax.shard_map(
        per_device,
        mesh=mesh,
        in_specs=placed,
        out_specs=(
            P("ep", None, "fsdp"),
            P("ep", None, "fsdp"),
            P("ep", "fsdp", None),
            P("ep", "fsdp"),
            P("ep", "fsdp"),
            P("ep", "fsdp"),
            P(),
        ),
        check_vma=False,
    )
```

```python
import jax
import jax.numpy as jnp
from jax import lax
from jax.experimental import pallas as pl
from jax.experimental.pallas import tpu as pltpu
from jax.sharding import PartitionSpec as P

MESH = pl.DeviceIdType.MESH
N = 32
EP = 8
E, D, J = 8, 64, 1408
JT = J // 128
JD = J // N
ROWS = JD * E // 2
CJ = 128 // E
LINES = -(-JD // CJ)
WIDE = J + 128
FAR_FIRST = (4, 3, 5, 2, 6, 1, 7, 0)
ARRIVAL = (0, 4, 3, 5, 2, 6, 1, 7)
TILES = (4, 7, 3, 8, 5, 6, 2, 9, 1, 10, 0)
EARLY = 2

LEVELS, STEPS, LOWEST = 30720, 128, 120


def encode(x, per_unit):
    n = jnp.floor(jnp.abs(x) * per_unit + 0.5)
    high = jnp.floor(n * (1 / STEPS))
    v = jnp.exp2(high - LOWEST) * (1.0 + (n - STEPS * high) * (1 / STEPS))
    return jnp.where(x < 0, -v, v)


def decode(v):
    size = jnp.abs(v)
    high = jnp.floor(jnp.log2(size))
    n = (high + (LOWEST - 1.0)) * STEPS + size * jnp.exp2(-high) * STEPS
    return jnp.where(v < 0, -n, n)


def listed(values, i):
    found = 0
    for at, value in enumerate(values):
        found = jnp.where(i == at, value, found)
    return found


def exchange(
    gate, up, down, rw, rg, gate_out, up_out, down_out, scales, router,
    x, stage, sent, land, rows, tops, spread, recip, lines, got_lines, inv, fac, rw_v, rg_v, rhalf, rtile,
    tile_sem, load_sem, rload, lsend, lrecv, dsend, drecv, dself,
    csend, crecv, zsend, zrecv, ysend, yrecv, esend, erecv, eself,
):
    me = lax.axis_index("fsdp")
    ep = lax.axis_index("ep")
    z, yh, core = me // 4, lax.rem(me // 2, 2), lax.rem(me, 2)
    first = (JT * me) // N
    lane = lax.broadcasted_iota(jnp.int32, (E, 128), 1)
    row = lax.broadcasted_iota(jnp.int32, (E, 128), 0)

    barrier = pltpu.get_barrier_semaphore()
    for d in range(N - 1):
        to = lax.rem(me + 1 + (d + N // 3) % (N - 1), N)
        pl.semaphore_signal(barrier, inc=1, device_id={"fsdp": to}, device_id_type=MESH)
    for d in range(1, EP):
        pl.semaphore_signal(barrier, inc=1, device_id={"ep": lax.rem(ep + d, EP)}, device_id_type=MESH)

    def tile_at(i):
        return pl.multiple_of(lax.rem(first + listed(TILES, i), JT) * 128, 128)

    def tile_load(i):
        part = pl.ds(tile_at(i), 128)
        return pltpu.make_async_copy(gate.at[:, :, part], x.at[0, :, :, part], tile_sem.at[jnp.minimum(i, EARLY)])

    lax.fori_loop(0, JT, lambda i, _: (tile_load(i).start(), 0)[1], 0)
    loads = [pltpu.make_async_copy(ref, x.at[m], load_sem.at[m - 1]) for m, ref in ((1, up), (2, down))]
    for load in loads:
        load.start()
    rloads = [pltpu.make_async_copy(a, b, rload.at[i]) for i, (a, b) in enumerate(((rw, rw_v), (rg, rg_v)))]
    for load in rloads:
        load.start()

    def wait_bytes(ref, sem):
        pltpu.make_async_copy(ref, ref, sem).wait()

    def maxima(m):
        def one(e, _):
            tops[m, pl.ds(e, 1), :J] = jnp.max(jnp.abs(x[m, e]), axis=0, keepdims=True)
            return 0

        tops[m, :, J:] = jnp.zeros((E, WIDE - J), jnp.float32)
        lax.fori_loop(0, E, one, 0)

    def per_unit(top):
        return jnp.where(top > 1e-30, LEVELS / jnp.maximum(top, 1e-30), 0.0)

    def scaling(m):
        recip[...] = per_unit(tops[m])

    def lay_out(m, at):
        for r in range(E // 2):
            v = encode(x[m, 2 * r : 2 * r + 2, :, pl.ds(at, 128)], recip[2 * r : 2 * r + 2, pl.ds(at, 128)][:, None, :])
            stage[pl.ds(r, 128, stride=E // 2), :] = v.reshape(128, 128).T
        sent[m, pl.ds(pl.multiple_of(4 * at, 512), 512), :] = stage[...].astype(jnp.bfloat16)

    def first_tile(i):
        at = tile_at(i)
        top = jnp.max(jnp.abs(x[0, :, :, pl.ds(at, 128)]), axis=1)
        tops[0, :, pl.ds(at, 128)] = top
        recip[:, pl.ds(at, 128)] = per_unit(top)
        lay_out(0, at)

    def rows_of(m, to):
        return sent.at[m, pl.ds(pl.multiple_of(to * ROWS, ROWS), ROWS)]

    def send_rows(m, to):
        @pl.when(to != me)
        def _():
            pltpu.make_async_remote_copy(
                rows_of(m, to), land.at[m, me], dsend.at[m], drecv.at[m + z if m == 2 else m], device_id={"fsdp": to}, device_id_type=MESH
            ).start()

        @pl.when(to == me)
        def _():
            pltpu.make_async_copy(rows_of(m, to), land.at[m, me], dself.at[m]).start()

    def first_to(q):
        return (N * q) // JT

    def spans(q):
        return (JT * first_to(q)) // N < q

    def send_first_tile(i):
        q = lax.rem(first + listed(TILES, i), JT)
        to = first_to(q)

        @pl.when(jnp.logical_not(spans(q)))
        def _():
            send_rows(0, to)

        for more in (1, 2):

            @pl.when(to + more < first_to(q + 1))
            def _():
                send_rows(0, to + more)

    def send_spanning(i):
        q = lax.rem(first + listed(TILES, i), JT)

        @pl.when(spans(q))
        def _():
            send_rows(0, first_to(q))

    def loop(start, stop, *steps):
        def one(i, _):
            for step in steps:
                step(i)
            return 0

        lax.fori_loop(start, stop, one, 0)

    def send_far_first(m):
        loop(0, JT, lambda i: lay_out(m, pl.multiple_of(i * 128, 128)))
        loop(0, N, lambda i: send_rows(m, 4 * lax.rem(z + listed(FAR_FIRST, i // 4), 8) + lax.rem(me + i, 4)))

    own_lanes = (lane // CJ) == row

    def draw_lines(m):
        for e in range(E):
            spread[e : e + 1, :] = pltpu.roll(tops[m, e : e + 1], CJ * e, 1)

        def one(to, _):
            for g in range(LINES):
                c0 = JD * to + CJ * g
                at = pl.multiple_of((c0 // 128) * 128, 128)
                near = pltpu.roll(spread[:, pl.ds(at, 256)], 256 - lax.rem(c0, 128), 1)[:, :128]
                g0 = (LINES * m + g) * 128
                lines[to, :, g0 : g0 + 128] = jnp.sum(jnp.where(own_lanes, near, 0.0), axis=0, keepdims=True)
            return 0

        lax.fori_loop(0, N, one, 0)

    tops[0, :, J:] = jnp.zeros((E, WIDE - J), jnp.float32)
    loop(0, EARLY, lambda i: tile_load(i).wait(), first_tile)
    rest = pl.ds(0, (JT - EARLY) * 128)
    pltpu.make_async_copy(gate.at[:, :, rest], x.at[0, :, :, rest], tile_sem.at[EARLY]).wait()
    pl.semaphore_wait(barrier, N - 1 + EP - 1)
    loop(0, EARLY, send_first_tile)
    loop(EARLY, JT, first_tile, send_first_tile)
    loop(0, JT, send_spanning)

    for load in rloads:
        load.wait()
    part = rw_v[...] * rg_v[...]
    rhalf[0] = jnp.concatenate([part, part], axis=1)
    router_core = pltpu.make_async_remote_copy(
        rhalf.at[0], rhalf.at[1], csend, crecv, device_id={"fsdp": me + 1 - 2 * core}, device_id_type=MESH
    )
    router_core.start()
    loads[0].wait()
    loads[1].wait()
    maxima(1)
    maxima(2)
    draw_lines(0)
    draw_lines(1)
    draw_lines(2)
    got_lines[me] = lines[me]

    def send_line(d, _):
        to = lax.rem(me + d, N)
        pltpu.make_async_remote_copy(
            lines.at[to], got_lines.at[me], lsend, lrecv, device_id={"fsdp": to}, device_id_type=MESH
        ).start()
        return 0

    lax.fori_loop(1, N, send_line, 0)

    router_core.wait()
    own_side = (lane // 64) == core
    rtile[yh, z] = jnp.where(own_side, rhalf[0], rhalf[1]).astype(jnp.bfloat16)

    def router_z(d, _):
        pltpu.make_async_remote_copy(
            rtile.at[yh, z], rtile.at[yh, z], zsend, zrecv,
            device_id={"fsdp": lax.rem(me + 4 * d, N)}, device_id_type=MESH,
        ).start()
        return 0

    lax.fori_loop(1, 8, router_z, 0)

    scaling(1)
    send_far_first(1)

    scaling(2)
    send_far_first(2)
    wait_bytes(rtile.at[0, pl.ds(0, 7)], zrecv)
    router_y = pltpu.make_async_remote_copy(
        rtile.at[yh], rtile.at[yh], ysend, yrecv, device_id={"fsdp": me + 2 - 4 * yh}, device_id_type=MESH
    )
    router_y.start()
    wait_bytes(got_lines.at[pl.ds(0, N - 1)], lrecv)
    router_y.wait_recv()

    def router_ep(d, _):
        for half in range(2):
            pltpu.make_async_remote_copy(
                rtile.at[half], router.at[ep, :, half], esend, erecv,
                device_id={"ep": lax.rem(ep + d, EP)}, device_id_type=MESH,
            ).start()
        return 0

    lax.fori_loop(1, EP, router_ep, 0)
    for half in range(2):
        pltpu.make_async_copy(rtile.at[half], router.at[ep, :, half], eself.at[half]).start()

    def side_by_side(a, b):
        low = lax.broadcasted_iota(jnp.int32, (ROWS, 128), 1) < 64
        rows[pl.ds(0, ROWS, stride=2), :] = jnp.where(low, a, pltpu.roll(b, 64, 1))
        rows[pl.ds(1, ROWS, stride=2), :] = jnp.where(low, pltpu.roll(a, 64, 1), b)
        return rows[...]

    def by_expert(line):
        line = jnp.broadcast_to(line, (E, 128))
        for_each = line
        for e in range(1, E):
            for_each = jnp.where(row == e, pltpu.roll(line, 128 - CJ * e, 1), for_each)
        return for_each

    def line_at(m, g):
        return pl.ds((LINES * m + g) * 128, 128)

    def await_last(i, plane):
        @pl.when(jnp.logical_and(i % 2 == 0, plane == z))
        def _():
            wait_bytes(land.at[2, pl.ds(0, 3)], drecv.at[2 + plane])

        @pl.when(jnp.logical_and(i % 2 == 0, plane != z))
        def _():
            wait_bytes(land.at[2, pl.ds(0, 4)], drecv.at[2 + plane])

    def merge(m, out):
        scale = jnp.zeros((E, 128), jnp.float32)
        for g in range(LINES):
            part = by_expert(jnp.max(got_lines[:, :, line_at(m, g)], axis=0))
            inv[g] = (1 / LEVELS) / jnp.where(part > 0, part, 1.0)
            scale = jnp.where(lane // CJ == g, pltpu.roll(part, CJ * g, 1), scale)
        scales[m] = scale
        if m < 2:
            wait_bytes(land.at[m, pl.ds(0, N - 1)], drecv.at[m])
        pltpu.make_async_copy(rows_of(m, me), land.at[m, me], dself.at[m]).wait()
        low = lane < 64

        def chip(i, _):
            c = 2 * lax.rem(z + listed(ARRIVAL, i // 2), 8) + lax.rem(yh + i, 2)
            for g in range(LINES):
                per = [
                    by_expert(got_lines[2 * c + side, :, line_at(m, g)]) * inv[g] for side in range(2)
                ]
                for j in range(min(CJ, JD - CJ * g)):
                    a, b = (jnp.broadcast_to(p[:, j : j + 1], (E, 128)) for p in per)
                    fac[(CJ * g + j) * E : (CJ * g + j + 1) * E, :] = jnp.where(low, a, b)
            if m == 2:
                await_last(i, c // 2)
            a, b = (decode(land[m, 2 * c + side].astype(jnp.float32)) for side in range(2))
            v = (side_by_side(a, b) * fac[...]).astype(jnp.bfloat16)
            out[:, :, pl.ds(pl.multiple_of(c * 128, 128), 128)] = v.reshape(JD, E, 128)
            return 0

        lax.fori_loop(0, N // 2, chip, 0)

    merge(0, gate_out)
    wait_bytes(rtile.at[0, pl.ds(0, 7)], zsend)
    router_y.wait_send()
    wait_bytes(router.at[pl.ds(0, EP - 1)], esend)
    wait_bytes(router.at[pl.ds(0, EP - 1)], erecv)
    for half in range(2):
        pltpu.make_async_copy(rtile.at[half], router.at[ep, :, half], eself.at[half]).wait()
    merge(1, up_out)
    merge(2, down_out)
    wait_bytes(lines.at[pl.ds(0, N - 1)], lsend)
    for m in range(3):
        wait_bytes(sent.at[m, pl.ds(0, (N - 1) * ROWS)], dsend.at[m])


def finish(gate, up, down, scales, router, gate_out, up_out, down_out, sg, su, sd, router_out, cut, sem):
    copies = [
        pltpu.make_async_copy(a, b, sem.at[i])
        for i, (a, b) in enumerate(((gate, gate_out), (up, up_out), (down, down_out), (router, router_out)))
    ]
    for copy in copies:
        copy.start()
    cut[...] = scales[:, :, :JD]
    small = [pltpu.make_async_copy(cut.at[m], out, sem.at[4 + m]) for m, out in enumerate((sg, su, sd))]
    for copy in small:
        copy.start()
    for copy in copies + small:
        copy.wait()


def per_device(train_gate, train_up, train_down, router_weight, router_gain):
    f32, bf16 = jnp.float32, jnp.bfloat16
    hbm = pl.BlockSpec(memory_space=pltpu.HBM)
    vmem = pl.BlockSpec(memory_space=pltpu.VMEM)
    dma = pltpu.SemaphoreType.DMA

    def stay(a):
        return pltpu.with_memory_space_constraint(a, pltpu.HBM)

    ready = jax.ShapeDtypeStruct((JD, E, D * N), bf16)
    gate, up, down, scales, router = pl.pallas_call(
        exchange,
        out_shape=(
            *(ready,) * 3,
            jax.ShapeDtypeStruct((3, E, 128), f32),
            jax.ShapeDtypeStruct((EP, 8, 2, E, 128), bf16),
        ),
        in_specs=[hbm] * 5,
        out_specs=(vmem,) * 5,
        scratch_shapes=[
            pltpu.VMEM((3, E, D, J), f32),
            pltpu.VMEM((512, 128), f32),
            pltpu.VMEM((3, N * ROWS, 128), bf16),
            pltpu.VMEM((3, N, ROWS, 128), bf16),
            pltpu.VMEM((JD * E, 128), f32),
            pltpu.VMEM((3, E, WIDE), f32),
            pltpu.VMEM((E, WIDE), f32),
            pltpu.VMEM((E, WIDE), f32),
            pltpu.VMEM((N, 1, 3 * LINES * 128), f32),
            pltpu.VMEM((N, 1, 3 * LINES * 128), f32),
            pltpu.VMEM((LINES, E, 128), f32),
            pltpu.VMEM((JD * E, 128), f32),
            pltpu.VMEM((E, D), f32),
            pltpu.VMEM((1, D), f32),
            pltpu.VMEM((2, E, 128), f32),
            pltpu.VMEM((2, 8, E, 128), bf16),
        ]
        + [dma((EARLY + 1,)), dma((2,)), dma((2,))]
        + [dma] * 2
        + [dma((3,)), dma((2 + 8,)), dma((3,))]
        + [dma] * 8
        + [dma((2,))],
        compiler_params=pltpu.CompilerParams(collective_id=0, has_side_effects=True, vmem_limit_bytes=40 * 2**20),
        name="exchange",
    )(
        stay(train_gate),
        stay(train_up),
        stay(jnp.transpose(train_down, (0, 2, 1))),
        stay(jnp.transpose(router_weight)),
        stay(router_gain[None, :]),
    )
    scale = jax.ShapeDtypeStruct((E, JD), f32)
    gate, up, down, scale_gate, scale_up, scale_down, router = pl.pallas_call(
        finish,
        out_shape=(*(ready,) * 3, *(scale,) * 3, jax.ShapeDtypeStruct((EP, 8, 2, E, 128), bf16)),
        in_specs=[vmem] * 5,
        out_specs=(hbm,) * 7,
        scratch_shapes=[pltpu.VMEM((3, E, JD), f32), dma((7,))],
        compiler_params=pltpu.CompilerParams(vmem_limit_bytes=16 * 2**20),
        name="finish",
    )(gate, up, down, scales, router)
    serve = jnp.transpose(router, (0, 3, 1, 2, 4)).reshape(EP * E, D * N)
    return (
        jnp.transpose(gate, (1, 2, 0)),
        jnp.transpose(up, (1, 2, 0)),
        jnp.transpose(down, (1, 0, 2)),
        scale_gate,
        scale_up,
        scale_down,
        jnp.transpose(serve),
    )


def solution(mesh):
    placed = (
        P("ep", "fsdp", None),
        P("ep", "fsdp", None),
        P("ep", None, "fsdp"),
        P("fsdp", "ep"),
        P("fsdp"),
    )
    return jax.shard_map(
        per_device,
        mesh=mesh,
        in_specs=placed,
        out_specs=(
            P("ep", None, "fsdp"),
            P("ep", None, "fsdp"),
            P("ep", "fsdp", None),
            P("ep", "fsdp"),
            P("ep", "fsdp"),
            P("ep", "fsdp"),
            P(),
        ),
        check_vma=False,
    )
```

```python
import jax
import jax.numpy as jnp
from jax import lax
from jax.experimental import pallas as pl
from jax.experimental.pallas import tpu as pltpu
from jax.sharding import PartitionSpec as P

MESH = pl.DeviceIdType.MESH
N = 32
EP = 8
E, D, J = 8, 64, 1408
JT = J // 128
JD = J // N
ROWS = JD * E // 2
CJ = 128 // E
LINES = -(-JD // CJ)
WIDE = J + 128
FAR_FIRST = (4, 3, 5, 2, 6, 1, 7, 0)
ARRIVAL = (0, 4, 3, 5, 2, 6, 1, 7)
TILES = (4, 7, 3, 8, 5, 6, 2, 9, 1, 10, 0)
EARLY = 2

LEVELS, STEPS, LOWEST = 30720, 128, 120


def encode(x, per_unit):
    n = jnp.floor(jnp.abs(x) * per_unit + 0.5)
    high = jnp.floor(n * (1 / STEPS))
    v = jnp.exp2(high - LOWEST) * (1.0 + (n - STEPS * high) * (1 / STEPS))
    return jnp.where(x < 0, -v, v)


def decode(v):
    size = jnp.abs(v)
    high = jnp.floor(jnp.log2(size))
    n = (high + (LOWEST - 1.0)) * STEPS + size * jnp.exp2(-high) * STEPS
    return jnp.where(v < 0, -n, n)


def listed(values, i):
    found = 0
    for at, value in enumerate(values):
        found = jnp.where(i == at, value, found)
    return found


def exchange(
    gate, up, down, rw, rg, gate_out, up_out, down_out, scales, router,
    x, stage, sent, land, rows, tops, spread, recip, others, lines, got_lines, chip_lines, got_chip_lines, inv, fac, rw_v, rg_v, rhalf, rtile,
    tile_sem, load_sem, rload, osend, orecv, lsend, lrecv, dsend, drecv, dself,
    csend, crecv, zsend, zrecv, ysend, yrecv, esend, erecv, eself,
):
    me = lax.axis_index("fsdp")
    ep = lax.axis_index("ep")
    z, yh, core = me // 4, lax.rem(me // 2, 2), lax.rem(me, 2)
    first = (JT * me) // N
    lane = lax.broadcasted_iota(jnp.int32, (E, 128), 1)
    row = lax.broadcasted_iota(jnp.int32, (E, 128), 0)

    barrier = pltpu.get_barrier_semaphore()
    for d in range(N - 1):
        to = lax.rem(me + 1 + (d + N // 3) % (N - 1), N)
        pl.semaphore_signal(barrier, inc=1, device_id={"fsdp": to}, device_id_type=MESH)
    for d in range(1, EP):
        pl.semaphore_signal(barrier, inc=1, device_id={"ep": lax.rem(ep + d, EP)}, device_id_type=MESH)

    def tile_at(i):
        return pl.multiple_of(lax.rem(first + listed(TILES, i), JT) * 128, 128)

    def tile_load(i):
        part = pl.ds(tile_at(i), 128)
        return pltpu.make_async_copy(gate.at[:, :, part], x.at[0, :, :, part], tile_sem.at[jnp.minimum(i, EARLY)])

    lax.fori_loop(0, JT, lambda i, _: (tile_load(i).start(), 0)[1], 0)
    loads = [pltpu.make_async_copy(ref, x.at[m], load_sem.at[m - 1]) for m, ref in ((1, up), (2, down))]
    for load in loads:
        load.start()
    rloads = [pltpu.make_async_copy(a, b, rload.at[i]) for i, (a, b) in enumerate(((rw, rw_v), (rg, rg_v)))]
    for load in rloads:
        load.start()

    def wait_bytes(ref, sem):
        pltpu.make_async_copy(ref, ref, sem).wait()

    def maxima(m):
        def one(e, _):
            tops[m, pl.ds(e, 1), :J] = jnp.max(jnp.abs(x[m, e]), axis=0, keepdims=True)
            return 0

        tops[m, :, J:] = jnp.zeros((E, WIDE - J), jnp.float32)
        lax.fori_loop(0, E, one, 0)

    def per_unit(top):
        return jnp.where(top > 1e-30, LEVELS / jnp.maximum(top, 1e-30), 0.0)

    def scaling(m):
        recip[...] = per_unit(tops[m])

    def lay_out(m, at):
        for r in range(E // 2):
            v = encode(x[m, 2 * r : 2 * r + 2, :, pl.ds(at, 128)], recip[2 * r : 2 * r + 2, pl.ds(at, 128)][:, None, :])
            stage[pl.ds(r, 128, stride=E // 2), :] = v.reshape(128, 128).T
        sent[m, pl.ds(pl.multiple_of(4 * at, 512), 512), :] = stage[...].astype(jnp.bfloat16)

    def first_tile(i):
        at = tile_at(i)
        top = jnp.max(jnp.abs(x[0, :, :, pl.ds(at, 128)]), axis=1)
        tops[0, :, pl.ds(at, 128)] = top
        recip[:, pl.ds(at, 128)] = per_unit(top)
        lay_out(0, at)

    def rows_of(m, to):
        return sent.at[m, pl.ds(pl.multiple_of(to * ROWS, ROWS), ROWS)]

    def send_rows(m, to):
        @pl.when(to != me)
        def _():
            pltpu.make_async_remote_copy(
                rows_of(m, to), land.at[m, me], dsend.at[m], drecv.at[m + z if m == 2 else m], device_id={"fsdp": to}, device_id_type=MESH
            ).start()

        @pl.when(to == me)
        def _():
            pltpu.make_async_copy(rows_of(m, to), land.at[m, me], dself.at[m]).start()

    def first_to(q):
        return (N * q) // JT

    def spans(q):
        return (JT * first_to(q)) // N < q

    def send_first_tile(i):
        q = lax.rem(first + listed(TILES, i), JT)
        to = first_to(q)

        @pl.when(jnp.logical_not(spans(q)))
        def _():
            send_rows(0, to)

        for more in (1, 2):

            @pl.when(to + more < first_to(q + 1))
            def _():
                send_rows(0, to + more)

    def send_spanning(i):
        q = lax.rem(first + listed(TILES, i), JT)

        @pl.when(spans(q))
        def _():
            send_rows(0, first_to(q))

    def loop(start, stop, *steps):
        def one(i, _):
            for step in steps:
                step(i)
            return 0

        lax.fori_loop(start, stop, one, 0)

    def send_far_first(m):
        loop(0, JT, lambda i: lay_out(m, pl.multiple_of(i * 128, 128)))
        loop(0, N, lambda i: send_rows(m, 4 * lax.rem(z + listed(FAR_FIRST, i // 4), 8) + lax.rem(me + i, 4)))

    own_lanes = (lane // CJ) == row

    def draw_lines(m):
        for e in range(E):
            spread[e : e + 1, :] = pltpu.roll(tops[m, e : e + 1], CJ * e, 1)

        def one(i, _):
            to, out = (i, lines.at[i]) if m == 0 else (2 * i + core, chip_lines.at[i])
            for g in range(LINES):
                c0 = JD * to + CJ * g
                at = pl.multiple_of((c0 // 128) * 128, 128)
                near = pltpu.roll(spread[:, pl.ds(at, 256)], 256 - lax.rem(c0, 128), 1)[:, :128]
                out[:, line_at(m, g)] = jnp.sum(jnp.where(own_lanes, near, 0.0), axis=0, keepdims=True)
            return 0

        lax.fori_loop(0, N if m == 0 else N // 2, one, 0)

    def line_at(m, g):
        return pl.ds((LINES * max(m - 1, 0) + g) * 128, 128)

    tops[0, :, J:] = jnp.zeros((E, WIDE - J), jnp.float32)
    loop(0, EARLY, lambda i: tile_load(i).wait(), first_tile)
    rest = pl.ds(0, (JT - EARLY) * 128)
    pltpu.make_async_copy(gate.at[:, :, rest], x.at[0, :, :, rest], tile_sem.at[EARLY]).wait()
    pl.semaphore_wait(barrier, N - 1 + EP - 1)
    loop(0, EARLY, send_first_tile)
    loop(EARLY, JT, first_tile, send_first_tile)
    loop(0, JT, send_spanning)

    for load in rloads:
        load.wait()
    part = rw_v[...] * rg_v[...]
    rhalf[0] = jnp.concatenate([part, part], axis=1)
    router_core = pltpu.make_async_remote_copy(
        rhalf.at[0], rhalf.at[1], csend, crecv, device_id={"fsdp": me + 1 - 2 * core}, device_id_type=MESH
    )
    router_core.start()
    loads[0].wait()
    loads[1].wait()
    maxima(1)
    maxima(2)
    pair = pltpu.make_async_remote_copy(
        tops.at[pl.ds(1, 2)], others, osend, orecv, device_id={"fsdp": me + 1 - 2 * core}, device_id_type=MESH
    )
    pair.start()
    draw_lines(0)
    got_lines[me] = lines[me]

    def send_line(d):
        to = lax.rem(me + d, N)
        pltpu.make_async_remote_copy(
            lines.at[to], got_lines.at[me], lsend.at[0], lrecv.at[0], device_id={"fsdp": to}, device_id_type=MESH
        ).start()

    def send_chip_line(d):
        to = lax.rem(me // 2 + d, N // 2)
        pltpu.make_async_remote_copy(
            chip_lines.at[to], got_chip_lines.at[me // 2], lsend.at[1], lrecv.at[1],
            device_id={"fsdp": 2 * to + core}, device_id_type=MESH,
        ).start()

    loop(1, N, send_line)
    pair.wait()
    for m in (1, 2):
        tops[m] = jnp.maximum(tops[m], others[m - 1])
        draw_lines(m)
    got_chip_lines[me // 2] = chip_lines[me // 2]
    loop(1, N // 2, send_chip_line)

    router_core.wait()
    own_side = (lane // 64) == core
    rtile[yh, z] = jnp.where(own_side, rhalf[0], rhalf[1]).astype(jnp.bfloat16)

    def router_z(d, _):
        pltpu.make_async_remote_copy(
            rtile.at[yh, z], rtile.at[yh, z], zsend, zrecv,
            device_id={"fsdp": lax.rem(me + 4 * d, N)}, device_id_type=MESH,
        ).start()
        return 0

    lax.fori_loop(1, 8, router_z, 0)

    scaling(1)
    send_far_first(1)

    scaling(2)
    send_far_first(2)
    wait_bytes(rtile.at[0, pl.ds(0, 7)], zrecv)
    router_y = pltpu.make_async_remote_copy(
        rtile.at[yh], rtile.at[yh], ysend, yrecv, device_id={"fsdp": me + 2 - 4 * yh}, device_id_type=MESH
    )
    router_y.start()
    wait_bytes(got_lines.at[pl.ds(0, N - 1)], lrecv.at[0])
    wait_bytes(got_chip_lines.at[pl.ds(0, N // 2 - 1)], lrecv.at[1])
    router_y.wait_recv()

    def router_ep(d, _):
        for half in range(2):
            pltpu.make_async_remote_copy(
                rtile.at[half], router.at[ep, :, half], esend, erecv,
                device_id={"ep": lax.rem(ep + d, EP)}, device_id_type=MESH,
            ).start()
        return 0

    lax.fori_loop(1, EP, router_ep, 0)
    for half in range(2):
        pltpu.make_async_copy(rtile.at[half], router.at[ep, :, half], eself.at[half]).start()

    def side_by_side(a, b):
        low = lax.broadcasted_iota(jnp.int32, (ROWS, 128), 1) < 64
        rows[pl.ds(0, ROWS, stride=2), :] = jnp.where(low, a, pltpu.roll(b, 64, 1))
        rows[pl.ds(1, ROWS, stride=2), :] = jnp.where(low, pltpu.roll(a, 64, 1), b)
        return rows[...]

    def by_expert(line):
        line = jnp.broadcast_to(line, (E, 128))
        for_each = line
        for e in range(1, E):
            for_each = jnp.where(row == e, pltpu.roll(line, 128 - CJ * e, 1), for_each)
        return for_each

    def await_last(i, plane):
        @pl.when(jnp.logical_and(i % 2 == 0, plane == z))
        def _():
            wait_bytes(land.at[2, pl.ds(0, 3)], drecv.at[2 + plane])

        @pl.when(jnp.logical_and(i % 2 == 0, plane != z))
        def _():
            wait_bytes(land.at[2, pl.ds(0, 4)], drecv.at[2 + plane])

    def merge(m, out):
        scale = jnp.zeros((E, 128), jnp.float32)
        for g in range(LINES):
            part = by_expert(jnp.max((got_chip_lines if m else got_lines)[:, :, line_at(m, g)], axis=0))
            inv[g] = (1 / LEVELS) / jnp.where(part > 0, part, 1.0)
            scale = jnp.where(lane // CJ == g, pltpu.roll(part, CJ * g, 1), scale)
        scales[m] = scale
        if m < 2:
            wait_bytes(land.at[m, pl.ds(0, N - 1)], drecv.at[m])
        pltpu.make_async_copy(rows_of(m, me), land.at[m, me], dself.at[m]).wait()
        low = lane < 64

        def chip(i, _):
            c = 2 * lax.rem(z + listed(ARRIVAL, i // 2), 8) + lax.rem(yh + i, 2)
            for g in range(LINES):
                if m == 0:
                    got = [got_lines[2 * c + side, :, line_at(m, g)] for side in range(2)]
                else:
                    got = [got_chip_lines[c, :, line_at(m, g)]]
                per = [by_expert(line) * inv[g] for line in got]
                for j in range(min(CJ, JD - CJ * g)):
                    both = [jnp.broadcast_to(p[:, j : j + 1], (E, 128)) for p in per]
                    fac[(CJ * g + j) * E : (CJ * g + j + 1) * E, :] = jnp.where(low, both[0], both[-1])
            if m == 2:
                await_last(i, c // 2)
            a, b = (decode(land[m, 2 * c + side].astype(jnp.float32)) for side in range(2))
            v = (side_by_side(a, b) * fac[...]).astype(jnp.bfloat16)
            out[:, :, pl.ds(pl.multiple_of(c * 128, 128), 128)] = v.reshape(JD, E, 128)
            return 0

        lax.fori_loop(0, N // 2, chip, 0)

    merge(0, gate_out)
    wait_bytes(rtile.at[0, pl.ds(0, 7)], zsend)
    router_y.wait_send()
    wait_bytes(router.at[pl.ds(0, EP - 1)], esend)
    wait_bytes(router.at[pl.ds(0, EP - 1)], erecv)
    for half in range(2):
        pltpu.make_async_copy(rtile.at[half], router.at[ep, :, half], eself.at[half]).wait()
    merge(1, up_out)
    merge(2, down_out)
    wait_bytes(lines.at[pl.ds(0, N - 1)], lsend.at[0])
    wait_bytes(chip_lines.at[pl.ds(0, N // 2 - 1)], lsend.at[1])
    for m in range(3):
        wait_bytes(sent.at[m, pl.ds(0, (N - 1) * ROWS)], dsend.at[m])


def finish(gate, up, down, scales, router, gate_out, up_out, down_out, sg, su, sd, router_out, cut, sem):
    copies = [
        pltpu.make_async_copy(a, b, sem.at[i])
        for i, (a, b) in enumerate(((gate, gate_out), (up, up_out), (down, down_out), (router, router_out)))
    ]
    for copy in copies:
        copy.start()
    cut[...] = scales[:, :, :JD]
    small = [pltpu.make_async_copy(cut.at[m], out, sem.at[4 + m]) for m, out in enumerate((sg, su, sd))]
    for copy in small:
        copy.start()
    for copy in copies + small:
        copy.wait()


def per_device(train_gate, train_up, train_down, router_weight, router_gain):
    f32, bf16 = jnp.float32, jnp.bfloat16
    hbm = pl.BlockSpec(memory_space=pltpu.HBM)
    vmem = pl.BlockSpec(memory_space=pltpu.VMEM)
    dma = pltpu.SemaphoreType.DMA

    def stay(a):
        return pltpu.with_memory_space_constraint(a, pltpu.HBM)

    ready = jax.ShapeDtypeStruct((JD, E, D * N), bf16)
    gate, up, down, scales, router = pl.pallas_call(
        exchange,
        out_shape=(
            *(ready,) * 3,
            jax.ShapeDtypeStruct((3, E, 128), f32),
            jax.ShapeDtypeStruct((EP, 8, 2, E, 128), bf16),
        ),
        in_specs=[hbm] * 5,
        out_specs=(vmem,) * 5,
        scratch_shapes=[
            pltpu.VMEM((3, E, D, J), f32),
            pltpu.VMEM((512, 128), f32),
            pltpu.VMEM((3, N * ROWS, 128), bf16),
            pltpu.VMEM((3, N, ROWS, 128), bf16),
            pltpu.VMEM((JD * E, 128), f32),
            pltpu.VMEM((3, E, WIDE), f32),
            pltpu.VMEM((E, WIDE), f32),
            pltpu.VMEM((E, WIDE), f32),
            pltpu.VMEM((2, E, WIDE), f32),
            pltpu.VMEM((N, 1, LINES * 128), f32),
            pltpu.VMEM((N, 1, LINES * 128), f32),
            pltpu.VMEM((N // 2, 1, 2 * LINES * 128), f32),
            pltpu.VMEM((N // 2, 1, 2 * LINES * 128), f32),
            pltpu.VMEM((LINES, E, 128), f32),
            pltpu.VMEM((JD * E, 128), f32),
            pltpu.VMEM((E, D), f32),
            pltpu.VMEM((1, D), f32),
            pltpu.VMEM((2, E, 128), f32),
            pltpu.VMEM((2, 8, E, 128), bf16),
        ]
        + [dma((EARLY + 1,)), dma((2,)), dma((2,))]
        + [dma] * 2
        + [dma((2,))] * 2
        + [dma((3,)), dma((2 + 8,)), dma((3,))]
        + [dma] * 8
        + [dma((2,))],
        compiler_params=pltpu.CompilerParams(collective_id=0, has_side_effects=True, vmem_limit_bytes=40 * 2**20),
        name="exchange",
    )(
        stay(train_gate),
        stay(train_up),
        stay(jnp.transpose(train_down, (0, 2, 1))),
        stay(jnp.transpose(router_weight)),
        stay(router_gain[None, :]),
    )
    scale = jax.ShapeDtypeStruct((E, JD), f32)
    gate, up, down, scale_gate, scale_up, scale_down, router = pl.pallas_call(
        finish,
        out_shape=(*(ready,) * 3, *(scale,) * 3, jax.ShapeDtypeStruct((EP, 8, 2, E, 128), bf16)),
        in_specs=[vmem] * 5,
        out_specs=(hbm,) * 7,
        scratch_shapes=[pltpu.VMEM((3, E, JD), f32), dma((7,))],
        compiler_params=pltpu.CompilerParams(vmem_limit_bytes=16 * 2**20),
        name="finish",
    )(gate, up, down, scales, router)
    serve = jnp.transpose(router, (0, 3, 1, 2, 4)).reshape(EP * E, D * N)
    return (
        jnp.transpose(gate, (1, 2, 0)),
        jnp.transpose(up, (1, 2, 0)),
        jnp.transpose(down, (1, 0, 2)),
        scale_gate,
        scale_up,
        scale_down,
        jnp.transpose(serve),
    )


def solution(mesh):
    placed = (
        P("ep", "fsdp", None),
        P("ep", "fsdp", None),
        P("ep", None, "fsdp"),
        P("fsdp", "ep"),
        P("fsdp"),
    )
    return jax.shard_map(
        per_device,
        mesh=mesh,
        in_specs=placed,
        out_specs=(
            P("ep", None, "fsdp"),
            P("ep", None, "fsdp"),
            P("ep", "fsdp", None),
            P("ep", "fsdp"),
            P("ep", "fsdp"),
            P("ep", "fsdp"),
            P(),
        ),
        check_vma=False,
    )
```

```python
import jax
import jax.numpy as jnp
from jax import lax
from jax.experimental import pallas as pl
from jax.experimental.pallas import tpu as pltpu
from jax.sharding import PartitionSpec as P

MESH = pl.DeviceIdType.MESH
N = 32
EP = 8
E, D, J = 8, 64, 1408
JT = J // 128
JD = J // N
ROWS = JD * E // 2
CJ = 128 // E
LINES = -(-JD // CJ)
WIDE = J + 128
FAR_FIRST = (4, 3, 5, 2, 6, 1, 7, 0)
ARRIVAL = (0, 4, 3, 5, 2, 6, 1, 7)
TILES = (4, 7, 3, 8, 5, 6, 2, 9, 1, 10, 0)
EARLY = 2

LEVELS, STEPS, LOWEST = 30720, 128, 120


def encode(x, per_unit):
    n = jnp.floor(jnp.abs(x) * per_unit + 0.5)
    high = jnp.floor(n * (1 / STEPS))
    v = jnp.exp2(high - LOWEST) * (1.0 + (n - STEPS * high) * (1 / STEPS))
    return jnp.where(x < 0, -v, v)


def decode(v):
    size = jnp.abs(v)
    high = jnp.floor(jnp.log2(size))
    n = (high + (LOWEST - 1.0)) * STEPS + size * jnp.exp2(-high) * STEPS
    return jnp.where(v < 0, -n, n)


def listed(values, i):
    found = 0
    for at, value in enumerate(values):
        found = jnp.where(i == at, value, found)
    return found


def exchange(
    gate, up, down, rw, rg, gate_out, up_out, down_out, scales, router,
    x, stage, sent, land, rows, tops, spread, recip, others, lines, got_lines, chip_lines, got_chip_lines, inv, fac, rw_v, rg_v, rhalf, rtile,
    tile_sem, load_sem, rload, osend, orecv, lsend, lrecv, dsend, drecv, dself,
    csend, crecv, zsend, zrecv, ysend, yrecv, esend, erecv, eself,
):
    me = lax.axis_index("fsdp")
    ep = lax.axis_index("ep")
    z, yh, core = me // 4, lax.rem(me // 2, 2), lax.rem(me, 2)
    first = (JT * me) // N
    lane = lax.broadcasted_iota(jnp.int32, (E, 128), 1)
    row = lax.broadcasted_iota(jnp.int32, (E, 128), 0)

    barrier = pltpu.get_barrier_semaphore()
    for d in range(N - 1):
        to = lax.rem(me + 1 + (d + N // 3) % (N - 1), N)
        pl.semaphore_signal(barrier, inc=1, device_id={"fsdp": to}, device_id_type=MESH)
    for d in range(1, EP):
        pl.semaphore_signal(barrier, inc=1, device_id={"ep": lax.rem(ep + d, EP)}, device_id_type=MESH)

    def tile_at(i):
        return pl.multiple_of(lax.rem(first + listed(TILES, i), JT) * 128, 128)

    def tile_load(i):
        part = pl.ds(tile_at(i), 128)
        return pltpu.make_async_copy(gate.at[:, :, part], x.at[0, :, :, part], tile_sem.at[jnp.minimum(i, EARLY)])

    lax.fori_loop(0, JT, lambda i, _: (tile_load(i).start(), 0)[1], 0)
    loads = [pltpu.make_async_copy(ref, x.at[m], load_sem.at[m - 1]) for m, ref in ((1, up), (2, down))]
    for load in loads:
        load.start()
    rloads = [pltpu.make_async_copy(a, b, rload.at[i]) for i, (a, b) in enumerate(((rw, rw_v), (rg, rg_v)))]
    for load in rloads:
        load.start()

    def wait_bytes(ref, sem):
        pltpu.make_async_copy(ref, ref, sem).wait()

    def maxima(m):
        def one(e, _):
            tops[m, pl.ds(e, 1), :J] = jnp.max(jnp.abs(x[m, e]), axis=0, keepdims=True)
            return 0

        tops[m, :, J:] = jnp.zeros((E, WIDE - J), jnp.float32)
        lax.fori_loop(0, E, one, 0)

    def per_unit(top):
        return jnp.where(top > 1e-30, LEVELS / jnp.maximum(top, 1e-30), 0.0)

    def scaling(m):
        recip[...] = per_unit(tops[m])

    def lay_out(m, at):
        for r in range(E // 2):
            v = encode(x[m, 2 * r : 2 * r + 2, :, pl.ds(at, 128)], recip[2 * r : 2 * r + 2, pl.ds(at, 128)][:, None, :])
            stage[pl.ds(r, 128, stride=E // 2), :] = v.reshape(128, 128).T
        sent[m, pl.ds(pl.multiple_of(4 * at, 512), 512), :] = stage[...].astype(jnp.bfloat16)

    def first_tile(i):
        at = tile_at(i)
        top = jnp.max(jnp.abs(x[0, :, :, pl.ds(at, 128)]), axis=1)
        tops[0, :, pl.ds(at, 128)] = top
        recip[:, pl.ds(at, 128)] = per_unit(top)
        lay_out(0, at)

    def rows_of(m, to):
        return sent.at[m, pl.ds(pl.multiple_of(to * ROWS, ROWS), ROWS)]

    def send_rows(m, to):
        @pl.when(to != me)
        def _():
            pltpu.make_async_remote_copy(
                rows_of(m, to), land.at[m, me], dsend.at[m], drecv.at[m + z if m == 2 else m], device_id={"fsdp": to}, device_id_type=MESH
            ).start()

        @pl.when(to == me)
        def _():
            pltpu.make_async_copy(rows_of(m, to), land.at[m, me], dself.at[m]).start()

    def first_to(q):
        return (N * q) // JT

    def spans(q):
        return (JT * first_to(q)) // N < q

    def send_first_tile(i):
        q = lax.rem(first + listed(TILES, i), JT)
        to = first_to(q)

        @pl.when(jnp.logical_not(spans(q)))
        def _():
            send_rows(0, to)

        for more in (1, 2):

            @pl.when(to + more < first_to(q + 1))
            def _():
                send_rows(0, to + more)

    def send_spanning(i):
        q = lax.rem(first + listed(TILES, i), JT)

        @pl.when(spans(q))
        def _():
            send_rows(0, first_to(q))

    def loop(start, stop, *steps):
        def one(i, _):
            for step in steps:
                step(i)
            return 0

        lax.fori_loop(start, stop, one, 0)

    def send_far_first(m):
        loop(0, JT, lambda i: lay_out(m, pl.multiple_of(i * 128, 128)))
        loop(0, N, lambda i: send_rows(m, 4 * lax.rem(z + listed(FAR_FIRST, i // 4), 8) + lax.rem(me + i, 4)))

    own_lanes = (lane // CJ) == row

    def draw_lines(m):
        for e in range(E):
            spread[e : e + 1, :] = pltpu.roll(tops[m, e : e + 1], CJ * e, 1)

        def one(i, _):
            to, out = (i, lines.at[i]) if m == 0 else (2 * i + core, chip_lines.at[i])
            for g in range(LINES):
                c0 = JD * to + CJ * g
                at = pl.multiple_of((c0 // 128) * 128, 128)
                near = pltpu.roll(spread[:, pl.ds(at, 256)], 256 - lax.rem(c0, 128), 1)[:, :128]
                out[:, line_at(m, g)] = jnp.sum(jnp.where(own_lanes, near, 0.0), axis=0, keepdims=True)
            return 0

        lax.fori_loop(0, N if m == 0 else N // 2, one, 0)

    def line_at(m, g):
        return pl.ds((LINES * max(m - 1, 0) + g) * 128, 128)

    tops[0, :, J:] = jnp.zeros((E, WIDE - J), jnp.float32)
    loop(0, EARLY, lambda i: tile_load(i).wait(), first_tile)
    rest = pl.ds(0, (JT - EARLY) * 128)
    pltpu.make_async_copy(gate.at[:, :, rest], x.at[0, :, :, rest], tile_sem.at[EARLY]).wait()
    pl.semaphore_wait(barrier, N - 1 + EP - 1)
    loop(0, EARLY, send_first_tile)
    loop(EARLY, JT, first_tile, send_first_tile)
    loop(0, JT, send_spanning)

    for load in rloads:
        load.wait()
    part = rw_v[...] * rg_v[...]
    rhalf[0] = jnp.concatenate([part, part], axis=1)
    router_core = pltpu.make_async_remote_copy(
        rhalf.at[0], rhalf.at[1], csend, crecv, device_id={"fsdp": me + 1 - 2 * core}, device_id_type=MESH
    )
    router_core.start()
    loads[0].wait()
    loads[1].wait()
    maxima(1)
    maxima(2)
    pair = pltpu.make_async_remote_copy(
        tops.at[pl.ds(1, 2)], others, osend, orecv, device_id={"fsdp": me + 1 - 2 * core}, device_id_type=MESH
    )
    pair.start()
    draw_lines(0)
    got_lines[me] = lines[me]

    def send_line(d):
        to = lax.rem(me + d, N)
        pltpu.make_async_remote_copy(
            lines.at[to], got_lines.at[me], lsend.at[0], lrecv.at[0], device_id={"fsdp": to}, device_id_type=MESH
        ).start()

    def send_chip_line(d):
        to = lax.rem(me // 2 + d, N // 2)
        pltpu.make_async_remote_copy(
            chip_lines.at[to], got_chip_lines.at[me // 2], lsend.at[1], lrecv.at[1],
            device_id={"fsdp": 2 * to + core}, device_id_type=MESH,
        ).start()

    loop(1, N, send_line)
    pair.wait()
    for m in (1, 2):
        tops[m] = jnp.maximum(tops[m], others[m - 1])
        draw_lines(m)
    got_chip_lines[me // 2] = chip_lines[me // 2]
    loop(1, N // 2, send_chip_line)

    router_core.wait()
    own_side = (lane // 64) == core
    rtile[yh, z] = jnp.where(own_side, rhalf[0], rhalf[1]).astype(jnp.bfloat16)

    def router_z(d, _):
        pltpu.make_async_remote_copy(
            rtile.at[yh, z], rtile.at[yh, z], zsend, zrecv,
            device_id={"fsdp": lax.rem(me + 4 * d, N)}, device_id_type=MESH,
        ).start()
        return 0

    lax.fori_loop(1, 8, router_z, 0)

    scaling(1)
    send_far_first(1)

    scaling(2)
    send_far_first(2)
    wait_bytes(rtile.at[0, pl.ds(0, 7)], zrecv)
    router_y = pltpu.make_async_remote_copy(
        rtile.at[yh], rtile.at[yh], ysend, yrecv, device_id={"fsdp": me + 2 - 4 * yh}, device_id_type=MESH
    )
    router_y.start()
    wait_bytes(got_lines.at[pl.ds(0, N - 1)], lrecv.at[0])
    wait_bytes(got_chip_lines.at[pl.ds(0, N // 2 - 1)], lrecv.at[1])
    router_y.wait_recv()

    def router_ep(d, _):
        for half in range(2):
            pltpu.make_async_remote_copy(
                rtile.at[half], router.at[ep, :, half], esend, erecv,
                device_id={"ep": lax.rem(ep + d, EP)}, device_id_type=MESH,
            ).start()
        return 0

    lax.fori_loop(1, EP, router_ep, 0)
    for half in range(2):
        pltpu.make_async_copy(rtile.at[half], router.at[ep, :, half], eself.at[half]).start()

    def side_by_side(a, b):
        low = lax.broadcasted_iota(jnp.int32, (ROWS, 128), 1) < 64
        rows[pl.ds(0, ROWS, stride=2), :] = jnp.where(low, a, pltpu.roll(b, 64, 1))
        rows[pl.ds(1, ROWS, stride=2), :] = jnp.where(low, pltpu.roll(a, 64, 1), b)
        return rows[...]

    def by_expert(line):
        line = jnp.broadcast_to(line, (E, 128))
        for_each = line
        for e in range(1, E):
            for_each = jnp.where(row == e, pltpu.roll(line, 128 - CJ * e, 1), for_each)
        return for_each

    def await_last(plane):
        @pl.when(plane == z)
        def _():
            wait_bytes(land.at[2, pl.ds(0, 3)], drecv.at[2 + plane])

        @pl.when(plane != z)
        def _():
            wait_bytes(land.at[2, pl.ds(0, 4)], drecv.at[2 + plane])

    def merge(m, out):
        scale = jnp.zeros((E, 128), jnp.float32)
        for g in range(LINES):
            part = by_expert(jnp.max((got_chip_lines if m else got_lines)[:, :, line_at(m, g)], axis=0))
            inv[g] = (1 / LEVELS) / jnp.where(part > 0, part, 1.0)
            scale = jnp.where(lane // CJ == g, pltpu.roll(part, CJ * g, 1), scale)
        scales[m] = scale
        if m < 2:
            wait_bytes(land.at[m, pl.ds(0, N - 1)], drecv.at[m])
        pltpu.make_async_copy(rows_of(m, me), land.at[m, me], dself.at[m]).wait()
        low = lane < 64

        def units(c, u):
            for g in range(LINES):
                if m == 0:
                    got = [got_lines[2 * c + side, :, line_at(m, g)] for side in range(2)]
                else:
                    got = [got_chip_lines[c, :, line_at(m, g)]]
                per = [by_expert(line) * inv[g] for line in got]
                for j in range(min(CJ, JD - CJ * g)):
                    both = [jnp.broadcast_to(p[:, j : j + 1], (E, 128)) for p in per]
                    fac[u, (CJ * g + j) * E : (CJ * g + j + 1) * E, :] = jnp.where(low, both[0], both[-1])

        def plane(i, _):
            at = lax.rem(z + listed(ARRIVAL, i), 8)
            for u in range(2):
                units(2 * at + u, u)
            if m == 2:
                await_last(at)
            for u in range(2):
                c = 2 * at + u
                a, b = (decode(land[m, 2 * c + side].astype(jnp.float32)) for side in range(2))
                v = (side_by_side(a, b) * fac[u]).astype(jnp.bfloat16)
                out[:, :, pl.ds(pl.multiple_of(c * 128, 128), 128)] = v.reshape(JD, E, 128)
            return 0

        lax.fori_loop(0, 8, plane, 0)

    merge(0, gate_out)
    wait_bytes(rtile.at[0, pl.ds(0, 7)], zsend)
    router_y.wait_send()
    wait_bytes(router.at[pl.ds(0, EP - 1)], esend)
    wait_bytes(router.at[pl.ds(0, EP - 1)], erecv)
    for half in range(2):
        pltpu.make_async_copy(rtile.at[half], router.at[ep, :, half], eself.at[half]).wait()
    merge(1, up_out)
    merge(2, down_out)
    wait_bytes(lines.at[pl.ds(0, N - 1)], lsend.at[0])
    wait_bytes(chip_lines.at[pl.ds(0, N // 2 - 1)], lsend.at[1])
    for m in range(3):
        wait_bytes(sent.at[m, pl.ds(0, (N - 1) * ROWS)], dsend.at[m])


def finish(gate, up, down, scales, router, gate_out, up_out, down_out, sg, su, sd, router_out, cut, sem):
    copies = [
        pltpu.make_async_copy(a, b, sem.at[i])
        for i, (a, b) in enumerate(((gate, gate_out), (up, up_out), (down, down_out), (router, router_out)))
    ]
    for copy in copies:
        copy.start()
    cut[...] = scales[:, :, :JD]
    small = [pltpu.make_async_copy(cut.at[m], out, sem.at[4 + m]) for m, out in enumerate((sg, su, sd))]
    for copy in small:
        copy.start()
    for copy in copies + small:
        copy.wait()


def per_device(train_gate, train_up, train_down, router_weight, router_gain):
    f32, bf16 = jnp.float32, jnp.bfloat16
    hbm = pl.BlockSpec(memory_space=pltpu.HBM)
    vmem = pl.BlockSpec(memory_space=pltpu.VMEM)
    dma = pltpu.SemaphoreType.DMA

    def stay(a):
        return pltpu.with_memory_space_constraint(a, pltpu.HBM)

    ready = jax.ShapeDtypeStruct((JD, E, D * N), bf16)
    gate, up, down, scales, router = pl.pallas_call(
        exchange,
        out_shape=(
            *(ready,) * 3,
            jax.ShapeDtypeStruct((3, E, 128), f32),
            jax.ShapeDtypeStruct((EP, 8, 2, E, 128), bf16),
        ),
        in_specs=[hbm] * 5,
        out_specs=(vmem,) * 5,
        scratch_shapes=[
            pltpu.VMEM((3, E, D, J), f32),
            pltpu.VMEM((512, 128), f32),
            pltpu.VMEM((3, N * ROWS, 128), bf16),
            pltpu.VMEM((3, N, ROWS, 128), bf16),
            pltpu.VMEM((JD * E, 128), f32),
            pltpu.VMEM((3, E, WIDE), f32),
            pltpu.VMEM((E, WIDE), f32),
            pltpu.VMEM((E, WIDE), f32),
            pltpu.VMEM((2, E, WIDE), f32),
            pltpu.VMEM((N, 1, LINES * 128), f32),
            pltpu.VMEM((N, 1, LINES * 128), f32),
            pltpu.VMEM((N // 2, 1, 2 * LINES * 128), f32),
            pltpu.VMEM((N // 2, 1, 2 * LINES * 128), f32),
            pltpu.VMEM((LINES, E, 128), f32),
            pltpu.VMEM((2, JD * E, 128), f32),
            pltpu.VMEM((E, D), f32),
            pltpu.VMEM((1, D), f32),
            pltpu.VMEM((2, E, 128), f32),
            pltpu.VMEM((2, 8, E, 128), bf16),
        ]
        + [dma((EARLY + 1,)), dma((2,)), dma((2,))]
        + [dma] * 2
        + [dma((2,))] * 2
        + [dma((3,)), dma((2 + 8,)), dma((3,))]
        + [dma] * 8
        + [dma((2,))],
        compiler_params=pltpu.CompilerParams(collective_id=0, has_side_effects=True, vmem_limit_bytes=40 * 2**20),
        name="exchange",
    )(
        stay(train_gate),
        stay(train_up),
        stay(jnp.transpose(train_down, (0, 2, 1))),
        stay(jnp.transpose(router_weight)),
        stay(router_gain[None, :]),
    )
    scale = jax.ShapeDtypeStruct((E, JD), f32)
    gate, up, down, scale_gate, scale_up, scale_down, router = pl.pallas_call(
        finish,
        out_shape=(*(ready,) * 3, *(scale,) * 3, jax.ShapeDtypeStruct((EP, 8, 2, E, 128), bf16)),
        in_specs=[vmem] * 5,
        out_specs=(hbm,) * 7,
        scratch_shapes=[pltpu.VMEM((3, E, JD), f32), dma((7,))],
        compiler_params=pltpu.CompilerParams(vmem_limit_bytes=16 * 2**20),
        name="finish",
    )(gate, up, down, scales, router)
    serve = jnp.transpose(router, (0, 3, 1, 2, 4)).reshape(EP * E, D * N)
    return (
        jnp.transpose(gate, (1, 2, 0)),
        jnp.transpose(up, (1, 2, 0)),
        jnp.transpose(down, (1, 0, 2)),
        scale_gate,
        scale_up,
        scale_down,
        jnp.transpose(serve),
    )


def solution(mesh):
    placed = (
        P("ep", "fsdp", None),
        P("ep", "fsdp", None),
        P("ep", None, "fsdp"),
        P("fsdp", "ep"),
        P("fsdp"),
    )
    return jax.shard_map(
        per_device,
        mesh=mesh,
        in_specs=placed,
        out_specs=(
            P("ep", None, "fsdp"),
            P("ep", None, "fsdp"),
            P("ep", "fsdp", None),
            P("ep", "fsdp"),
            P("ep", "fsdp"),
            P("ep", "fsdp"),
            P(),
        ),
        check_vma=False,
    )
```
